128 devices in a mesh: dev: 2 (over y_hi), vert: 16 (over z, x), ha: 4 (over y_lo, core).
Axes of the slice: x: 4, y: 4 (y_hi: 2, y_lo: 2; y = y_hi * 2 + y_lo), z: 4, core: 2. Of those that a mesh axis runs over, the one named last changes fastest.
Arguments:
- teacher_logits: bfloat16 [2048, 128256], P(('dev', 'ha'), 'vert'), parts along dimension 0, may hold values from -40 to 260
- student_logits: bfloat16 [2048, 128256], P('dev', ('vert', 'ha')), parts along dimension 0, may hold values from -40 to 260
- targets: int32 [2048], P('dev'), parts along dimension 0, may hold values from 0 to 128255
- loss_mask: int32 [2048], P('dev'), parts along dimension 0, may hold values 0 or 1
- unembed: bfloat16 [128256, 4096], P(('vert', 'ha')), may hold values from -9 to 9
Outputs:
- hidden_grad: bfloat16 [2048, 4096], P(('dev', 'vert'), 'ha'), parts along dimension 0
The draws below stay inside these ranges and needn't reach their ends.
There are 2 independent parts, one for each index of `dev`. The reference program is written for one: setup_inputs(seed, part) draws one part's arguments, and reference() takes and returns one part's arrays. A program takes and returns all parts, laid end to end along the dimension named above; an argument that names none is the same for every part. Nothing has to cross between parts.
All inputs are finite; a program needn't handle non-finite values.
Results may differ from the reference program's by a relative error of at most 0.0034.
Values may be sent and summed in bfloat16 or wider, within the bound.
A program may use at most 128 MiB of HBM per device.

```python
import jax
import jax.numpy as jnp
from jax import lax

V = 128256
D = 4096
TOK = 1024


def logit_field(key, salt, spread):
    key_list = jax.random.split(jax.random.fold_in(key, salt), 1)
    values = jnp.clip(spread * jax.random.normal(key_list[0], (TOK, V), jnp.float32), -6.0 * spread, 6.0 * spread)
    return values.astype(jnp.bfloat16)


def draw_teacher_logits(key, part):
    return logit_field(key, 11, 4.5)


def draw_student_logits(key, part):
    return logit_field(key, 23, 3.0)


def draw_unembed(key, part):
    key_list = jax.random.split(jax.random.fold_in(key, 37), 2)
    rows = jnp.clip(jax.random.normal(key_list[0], (V, D), jnp.float32), -6.0, 6.0)
    common = 0.6 * jnp.clip(jax.random.normal(key_list[1], (1, D), jnp.float32), -4.0, 4.0)
    return (rows + common).astype(jnp.bfloat16)


def set_ends(array, stream_key, least, top_value):
    index_at = [jax.random.randint(jax.random.fold_in(stream_key, axis), (), 0, length) for axis, length in enumerate(array.shape)]
    main_axis = array.shape.index(max(array.shape))
    neighbour = index_at[:main_axis] + [(index_at[main_axis] + 1) % array.shape[main_axis]] + index_at[main_axis + 1:]
    return array.at[tuple(index_at)].set(least).at[tuple(neighbour)].set(top_value)


def setup_inputs(seed: int = 0, part: int = 0) -> dict:
    splits = jax.random.split(jax.random.key(seed), 6)
    own_keys = jax.random.split(jax.random.fold_in(splits[5], part), 6)
    teacher_logits = draw_teacher_logits(jax.random.fold_in(jax.random.fold_in(splits[5], part), 71), part)
    student_logits = draw_student_logits(jax.random.fold_in(jax.random.fold_in(splits[5], part), 71), part)
    targets = set_ends(jax.random.randint(own_keys[2], (TOK,), 0, V), jax.random.fold_in(own_keys[2], 1), 0, V - 1).astype(jnp.int32)
    loss_mask = set_ends((jax.random.randint(own_keys[3], (TOK,), 0, 4) < 3).astype(jnp.int32), jax.random.fold_in(own_keys[3], 1), 0, 1)
    unembed = draw_unembed(jax.random.fold_in(splits[5], 71), part)
    return {"teacher_logits": teacher_logits, "student_logits": student_logits, "targets": targets, "loss_mask": loss_mask, "unembed": unembed}


block_rows = 64


def log_total(values):
    top = jnp.max(values, axis=1)
    return top + jnp.log(jnp.sum(jnp.exp(values - top[:, None]), axis=1))


def reference(teacher_logits, student_logits, targets, loss_mask, unembed):
    count = TOK // block_rows

    def one_block(pieces):
        teach_vals, stud_vals, target_ids, mask_vals = pieces
        teach_vals = teach_vals.astype(jnp.float32)
        stud_vals = stud_vals.astype(jnp.float32)
        teach_prob = jnp.exp(teach_vals - log_total(teach_vals)[:, None]).astype(jnp.bfloat16)
        stud_prob = jnp.exp(stud_vals - log_total(stud_vals)[:, None])
        columns = jnp.arange(stud_vals.shape[1], dtype=jnp.int32)
        target_hot = (columns[None, :] == target_ids[:, None]).astype(jnp.float32)
        weight = mask_vals.astype(jnp.float32)[:, None]
        logit_grad = ((stud_prob - 0.5 * teach_prob.astype(jnp.float32) - 0.5 * target_hot) * weight).astype(jnp.bfloat16)
        return jnp.dot(logit_grad, unembed, preferred_element_type=jnp.float32).astype(jnp.bfloat16)

    blocks = lax.map(one_block, (teacher_logits.reshape(count, block_rows, V), student_logits.reshape(count, block_rows, V), targets.reshape(count, block_rows), loss_mask.reshape(count, block_rows)))
    return blocks.reshape(TOK, D)
```

```python
import functools

import jax
import jax.numpy as jnp
from jax import lax
from jax.experimental import pallas as pl
from jax.experimental.pallas import tpu as pltpu
from jax.sharding import PartitionSpec as P

MESH = pl.DeviceIdType.MESH
F32, BF16 = jnp.float32, jnp.bfloat16

TOK, DIM, WIDTH = 1024, 4096, 2004
VERT, HA, SIDE = 16, 4, 4
OWN = TOK // VERT
LANES = 2048
CHUNKS = 4
RPO = OWN // CHUNKS
ROWS = RPO * VERT
SENT = ROWS // HA
HALF = DIM // 2
TILE = 256
LOW = -1e30


def body(
    teach_ref, stud_ref, targ_ref, mask_ref, emb_ref, out_ref,
    emb, exch, grad, pair_out, pair_in, part, one_out, one_in, acc_one, two_in, acc_two, last_in,
    col_top, col_sum, col_targ, col_mask, col_tlse, col_slse, msg_one, got_one, msg_two, got_two,
    emb_sem, exch_send, exch_recv, stat_send, stat_recv, pair_send, pair_recv,
    one_send, one_recv, two_send, two_recv, last_send, last_recv,
):
    vert, ha = lax.axis_index("vert"), lax.axis_index("ha")
    core, ylo = lax.rem(ha, 2), ha // 2
    zpos, xpos = vert // SIDE, lax.rem(vert, SIDE)
    apos = xpos + core * (zpos - xpos)
    bpos = zpos + core * (xpos - zpos)
    step_a, step_b = 1 + 3 * core, 4 - 3 * core

    def to_ha(d):
        return {"ha": lax.rem(ha + d, HA)}

    def to_core():
        return {"ha": ha + 1 - 2 * core}

    def to_vert(e):
        return {"vert": lax.rem(vert + e, VERT)}

    def to_a(d):
        return {"vert": lax.rem(apos + d, SIDE) * step_a + bpos * step_b}

    def to_b(d):
        return {"vert": apos * step_a + lax.rem(bpos + d, SIDE) * step_b}

    def remote(src, dst, send, recv, target):
        return pltpu.make_async_remote_copy(
            src_ref=src, dst_ref=dst, send_sem=send, recv_sem=recv, device_id=target, device_id_type=MESH
        )

    barrier = pltpu.get_barrier_semaphore()
    for e in range(1, VERT):
        pl.semaphore_signal(barrier, inc=1, device_id=to_vert(e), device_id_type=MESH)
    for d in range(1, HA):
        pl.semaphore_signal(barrier, inc=1, device_id=to_ha(d), device_id_type=MESH)

    emb_copy = pltpu.make_async_copy(emb_ref, emb, emb_sem)
    emb_copy.start()

    lane = lax.broadcasted_iota(jnp.int32, (16, LANES), 1)
    inside = lane < WIDTH

    def local_stats(values):
        top = jnp.max(values, axis=1, keepdims=True)
        return top, jnp.sum(jnp.exp(values - top), axis=1, keepdims=True)

    def keep_stats(row, top, total):
        col_top[pl.ds(row, 16), :] = jnp.broadcast_to(top, (16, 128))
        col_sum[pl.ds(row, 16), :] = jnp.broadcast_to(total, (16, 128))

    def exch_copy(c, d):
        return remote(
            exch.at[c, 3 + d], exch.at[c, d], exch_send.at[c, d], exch_recv.at[c, d], to_ha(d)
        )

    def prepare(c):
        def group(q, carry):
            row = pl.multiple_of(q * OWN + c * RPO, 16)
            tops, sums = [], []
            for j in range(HA):
                first = j * WIDTH // 128 * 128
                shift = j * WIDTH - first
                span = LANES + (128 if shift + LANES > LANES and shift else 0)
                span = min(span, 63 * 128 - first)
                values = teach_ref[pl.ds(row, 16), first : first + span].astype(F32)
                if shift:
                    values = pltpu.roll(values, span - shift, 1)[:, :LANES]
                d = lax.rem(j + HA - ha, HA)
                place = d + 3 * ((d + 3) // 4)
                exch[c, place, pl.ds(pl.multiple_of(q * RPO, 16), 16), :] = values.astype(BF16)
                top, total = local_stats(jnp.where(inside, values, LOW))
                tops.append(top)
                sums.append(total)
            top = functools.reduce(jnp.maximum, tops)
            total = sum(s * jnp.exp(t - top) for s, t in zip(sums, tops))
            keep_stats(row, top, total)
            return carry

        lax.fori_loop(0, HA, group, 0)

    prepare(0)
    pl.semaphore_wait(barrier, VERT - 1 + HA - 1)
    for d in range(1, HA):
        exch_copy(0, d).start()
    for c in range(1, CHUNKS):
        prepare(c)

    eye = lax.broadcasted_iota(jnp.int32, (128, 128), 0) == lax.broadcasted_iota(jnp.int32, (128, 128), 1)

    def packed(ref, block):
        return jnp.sum(jnp.where(eye, ref[block * 128 : block * 128 + 128, :], 0.0), axis=0, keepdims=True)

    def unpack(ref, block, line):
        column = jnp.sum(jnp.where(eye, jnp.broadcast_to(line, (128, 128)), 0.0), axis=1, keepdims=True)
        ref[block * 128 : block * 128 + 128, :] = jnp.broadcast_to(column, (128, 128))

    for block in range(2):
        msg_one[16 + block : 17 + block, :] = packed(col_top, block)
        msg_one[18 + block : 19 + block, :] = packed(col_sum, block)
    msg_one[20:24, :] = jnp.zeros((4, 128), F32)

    def stud_group(g, carry):
        row = pl.multiple_of(g * 16, 16)
        values = jnp.where(inside, stud_ref[pl.ds(row, 16), :].astype(F32), LOW)
        keep_stats(row, *local_stats(values))
        return carry

    lax.fori_loop(0, TOK // 16, stud_group, 0)
    for block in range(8):
        msg_one[block : block + 1, :] = packed(col_top, block)
        msg_one[8 + block : 9 + block, :] = packed(col_sum, block)

    def stat_one(e):
        return remote(msg_one, got_one.at[e], stat_send.at[e], stat_recv.at[e], to_vert(e))

    for e in range(1, VERT):
        stat_one(e).start()
    for block in range(8):
        unpack(col_targ, block, targ_ref[block : block + 1, :].astype(F32))
        unpack(col_mask, block, mask_ref[block : block + 1, :].astype(F32))
    for e in range(1, VERT):
        stat_one(e).wait()

    def combined(get, count):
        tops, sums = zip(*(get(e) for e in range(count)))
        top = functools.reduce(jnp.maximum, tops)
        return top, sum(s * jnp.exp(t - top) for s, t in zip(sums, tops))

    def line_of(e, first, count):
        return msg_one[first : first + count, :] if e == 0 else got_one[e, first : first + count, :]

    stud_top, stud_sum = combined(lambda e: (line_of(e, 0, 8), line_of(e, 8, 8)), VERT)
    teach_top, teach_sum = combined(lambda e: (line_of(e, 16, 2), line_of(e, 18, 2)), VERT)
    teach_lse = teach_top + jnp.log(teach_sum)
    msg_two[0:8, :] = stud_top
    msg_two[8:16, :] = stud_sum
    for k in range(4):
        msg_two[16 + 2 * k : 18 + 2 * k, :] = teach_lse
    mine = lax.broadcasted_iota(jnp.int32, (8, 128), 0) // 2 == ha
    msg_two[16:24, :] = jnp.where(mine, msg_two[16:24, :], 0.0)

    def stat_two(d):
        return remote(msg_two, got_two.at[d], stat_send.at[VERT + d], stat_recv.at[VERT + d], to_ha(d))

    for d in range(1, HA):
        stat_two(d).start()
    for c in range(1, CHUNKS):
        for d in range(1, HA):
            exch_copy(c, d).start()
    for d in range(1, HA):
        stat_two(d).wait()

    def line_two(d, first):
        return msg_two[first : first + 8, :] if d == 0 else got_two[d, first : first + 8, :]

    stud_top, stud_sum = combined(lambda d: (line_two(d, 0), line_two(d, 8)), HA)
    stud_lse = stud_top + jnp.log(stud_sum)
    teach_lse = sum(line_two(d, 16) for d in range(HA))
    for block in range(8):
        unpack(col_slse, block, stud_lse[block : block + 1, :])
        unpack(col_tlse, block, teach_lse[block : block + 1, :])
    emb_copy.wait()

    offset = (vert * HA + ha) * WIDTH

    def pair_copy(c):
        return remote(pair_out.at[c % 2], pair_in.at[c % 2], pair_send.at[c], pair_recv.at[c], to_core())

    def one_copy(c, d):
        return remote(one_out.at[c, d], one_in.at[c, d], one_send.at[c, d], one_recv.at[c, d], to_a(d))

    def two_copy(c, d):
        there = pl.multiple_of(lax.rem(bpos + d, SIDE) * RPO, RPO)
        return remote(
            acc_one.at[c, pl.ds(there, RPO)], two_in.at[c, d], two_send.at[c, d], two_recv.at[c, d], to_b(d)
        )

    def last_copy(c):
        away = pl.multiple_of((1 - ylo) * (HALF // 2), 128)
        return remote(
            acc_two.at[c, :, pl.ds(away, HALF // 2)], last_in.at[c], last_send.at[c], last_recv.at[c], to_ha(2)
        )

    def product(c, which, dst):
        def step(n, carry):
            column = which * (DIM // 4) + (n // 4) * HALF + lax.rem(n, 4) * TILE
            dst[:, pl.ds(pl.multiple_of(n * TILE, TILE), TILE)] = jnp.dot(
                grad[:, :WIDTH], emb[:, pl.ds(pl.multiple_of(column, TILE), TILE)],
                preferred_element_type=F32,
            )
            return carry

        lax.fori_loop(0, HALF // TILE, step, 0)

    def multiply(c):
        for d in range(1, HA):
            exch_copy(c, d).wait()

        def group(v, carry):
            row = pl.multiple_of(v * OWN + c * RPO, 16)
            d = lax.rem(ha + HA - v // 4, HA)
            teach = exch[c, d, pl.ds(pl.multiple_of(lax.rem(v, 4) * RPO, 16), 16), :].astype(F32)
            prob = jnp.exp(teach - col_tlse[pl.ds(row, 16), 0:1]).astype(BF16).astype(F32)
            stud = jnp.exp(stud_ref[pl.ds(row, 16), :].astype(F32) - col_slse[pl.ds(row, 16), 0:1])
            at = col_targ[pl.ds(row, 16), 0:1].astype(jnp.int32) - offset
            hot = jnp.where(lane == at, 0.5, 0.0)
            value = (stud - 0.5 * prob - hot) * col_mask[pl.ds(row, 16), 0:1]
            grad[pl.ds(pl.multiple_of(v * RPO, 16), 16), :] = jnp.where(inside, value, 0.0).astype(BF16)
            return carry

        lax.fori_loop(0, VERT, group, 0)
        if c >= 2:
            pair_copy(c - 2).wait_send()
        product(c, 1 - core, pair_out.at[c % 2])
        pair_copy(c).start()
        product(c, core, part)

    def stage_one(c):
        pair_copy(c).wait_recv()
        for d in range(SIDE):
            owner = lax.rem(apos + d, SIDE) * step_a

            def rows_of(q, carry):
                row = pl.multiple_of((owner + q * step_b) * RPO, RPO)
                value = part[pl.ds(row, RPO), :] + pair_in[c % 2, pl.ds(row, RPO), :]
                to = pl.ds(pl.multiple_of(q * RPO, RPO), RPO)
                if d == 0:
                    acc_one[c, to, :] = value
                else:
                    one_out[c, d, to, :] = value.astype(BF16)
                return carry

            lax.fori_loop(0, SIDE, rows_of, 0)
        for d in range(1, SIDE):
            one_copy(c, d).start()

    def stage_two(c):
        for d in range(1, SIDE):
            one_copy(c, d).wait_recv()

        def rows_of(q, carry):
            at = pl.ds(pl.multiple_of(q * RPO, RPO), RPO)
            acc_one[c, at, :] = acc_one[c, at, :] + sum(
                one_in[c, d, at, :].astype(F32) for d in range(1, SIDE)
            )
            return carry

        lax.fori_loop(0, SIDE, rows_of, 0)
        for d in range(1, SIDE):
            two_copy(c, d).start()

    def stage_three(c):
        for d in range(1, SIDE):
            two_copy(c, d).wait_recv()
        here = pl.ds(pl.multiple_of(bpos * RPO, RPO), RPO)
        acc_two[c] = acc_one[c, here, :] + two_in[c, 1] + two_in[c, 2] + two_in[c, 3]
        last_copy(c).start()

    def finish(c):
        last_copy(c).wait_recv()
        here = pl.ds(pl.multiple_of(ylo * (HALF // 2), 128), HALF // 2)
        out_ref[c * RPO : c * RPO + RPO, :] = (acc_two[c, :, here] + last_in[c]).astype(BF16)

    for turn in range(CHUNKS + 3):
        if turn < CHUNKS:
            multiply(turn)
            stage_one(turn)
        if 0 <= turn - 1 < CHUNKS:
            stage_two(turn - 1)
        if 0 <= turn - 2 < CHUNKS:
            stage_three(turn - 2)
        if 0 <= turn - 3 < CHUNKS:
            finish(turn - 3)

    for c in range(CHUNKS):
        if c >= CHUNKS - 2:
            pair_copy(c).wait_send()
        for d in range(1, SIDE):
            one_copy(c, d).wait_send()
            two_copy(c, d).wait_send()
        last_copy(c).wait_send()


def on_device(teacher_logits, student_logits, targets, loss_mask, unembed):
    whole = lambda shape: pl.BlockSpec(shape, lambda i: (0,) * len(shape), pipeline_mode=pl.Buffered(1))
    dma = pltpu.SemaphoreType.DMA
    scratch = [
        pltpu.VMEM((WIDTH, DIM), BF16),
        pltpu.VMEM((CHUNKS, 7, SENT, LANES), BF16),
        pltpu.VMEM((ROWS, LANES), BF16),
        pltpu.VMEM((2, ROWS, HALF), F32),
        pltpu.VMEM((2, ROWS, HALF), F32),
        pltpu.VMEM((ROWS, HALF), F32),
        pltpu.VMEM((CHUNKS, SIDE, SIDE * RPO, HALF), BF16),
        pltpu.VMEM((CHUNKS, SIDE, SIDE * RPO, HALF), BF16),
        pltpu.VMEM((CHUNKS, SIDE * RPO, HALF), F32),
        pltpu.VMEM((CHUNKS, SIDE, RPO, HALF), F32),
        pltpu.VMEM((CHUNKS, RPO, HALF), F32),
        pltpu.VMEM((CHUNKS, RPO, HALF // 2), F32),
        *[pltpu.VMEM((TOK, 128), F32)] * 6,
        pltpu.VMEM((24, 128), F32),
        pltpu.VMEM((VERT, 24, 128), F32),
        pltpu.VMEM((24, 128), F32),
        pltpu.VMEM((HA, 24, 128), F32),
        dma,
        dma((CHUNKS, HA)), dma((CHUNKS, HA)),
        dma((VERT + HA,)), dma((VERT + HA,)),
        dma((CHUNKS,)), dma((CHUNKS,)),
        dma((CHUNKS, SIDE)), dma((CHUNKS, SIDE)),
        dma((CHUNKS, SIDE)), dma((CHUNKS, SIDE)),
        dma((CHUNKS,)), dma((CHUNKS,)),
    ]
    return pl.pallas_call(
        body,
        grid=(1,),
        out_shape=jax.ShapeDtypeStruct((OWN, DIM // HA), BF16),
        in_specs=[
            whole((TOK // HA, 63 * 128)),
            whole((TOK, LANES)),
            whole((8, 128)),
            whole((8, 128)),
            pl.BlockSpec(memory_space=pl.ANY),
        ],
        out_specs=pl.BlockSpec((OWN, DIM // HA), lambda i: (0, 0)),
        scratch_shapes=scratch,
        compiler_params=pltpu.CompilerParams(
            collective_id=0, has_side_effects=True, vmem_limit_bytes=67043328
        ),
    )(teacher_logits, student_logits, targets.reshape(8, 128), loss_mask.reshape(8, 128), unembed)


def solution(mesh):
    placed = (
        P(("dev", "ha"), "vert"),
        P("dev", ("vert", "ha")),
        P("dev"),
        P("dev"),
        P(("vert", "ha"), None),
    )
    return jax.shard_map(
        on_device, mesh=mesh, in_specs=placed, out_specs=P(("dev", "vert"), "ha"), check_vma=False
    )
```
